32 devices in a mesh: sector: 4 (over y, x), obl: 8 (over z, core).
Axes of the slice: x: 2, y: 2, z: 4, core: 2. Of those that a mesh axis runs over, the one named last changes fastest.
Arguments:
- spectrum: float32 [2, 8, 8, 65536], P(None, None, 'sector', 'obl'), may hold values from -6 to 6
- quantile_index: int32 [8], replicated, may hold values from 32768 to 64512
- bands: int32 [131072], P(('sector', 'obl')), may hold values from 1 to 1024
- default_prob: float32 [131072], P(('sector', 'obl')), may hold values from 0.002 to 0.1
- weights: int32 [8, 131072], P(None, ('sector', 'obl')), may hold values from 0 to 8
- live_rows: int32 [4, 8], P('sector', 'obl'), may hold values from 1 to 4096, as said below
Outputs:
- obligor_contrib: float32 [8, 131072], P(None, ('sector', 'obl'))
- sector_share: float32 [8, 8], P(None, 'sector')
The draws below stay inside these ranges and needn't reach their ends.
Inputs may be any that keep to these rules, and one draw needn't show every extreme that they name: `live_rows`: in each row (the devices of one sector index), the entries sum to 8192; exactly one of them equals 4096.
All inputs are finite; a program needn't handle non-finite values.
Results may differ from the reference program's by a relative error of at most 0.00011.
Values sent between devices are 32-bit elements; how exact they have to be, the bound alone decides.
A program may use at most 64 MiB of HBM per device.

```python
import math
import jax
import jax.numpy as jnp
from jax import lax

GRID = 65536
BANDS = 1024
SCEN = 8
SECTORS = 8
OBL_DEV = 1024
CAP = 4096
SLOTS = 131072
OBLIGORS = 32768
N_SECTOR = 4
N_OBL = 8


def draw_live_rows(key, part):
    heavy_key, share_key = jax.random.split(jax.random.fold_in(key, 17))
    heavy_index = jax.random.randint(heavy_key, (N_SECTOR, 1), 0, N_OBL)
    spread = jax.random.randint(share_key, (N_SECTOR, N_OBL), 500, 1001)
    column = jnp.arange(N_OBL, dtype=jnp.int32)[None, :]
    is_heavy = column == heavy_index
    spread = jnp.where(is_heavy, 0, spread)
    remainder_rows = (N_OBL - 4) * OBL_DEV
    base_rows = 1 + (remainder_rows - (N_OBL - 1)) * spread // jnp.sum(spread, axis=1, keepdims=True)
    base_rows = jnp.where(is_heavy, 0, base_rows)
    leftover = remainder_rows - jnp.sum(base_rows, axis=1, keepdims=True)
    position = jnp.cumsum(jnp.where(is_heavy, 0, 1), axis=1) - 1
    extra_row = jnp.where(is_heavy, 0, (position < leftover).astype(jnp.int32))
    return jnp.where(is_heavy, 4 * OBL_DEV, base_rows + extra_row).astype(jnp.int32)


def with_ends(values, own_key, least, top_value):
    index_at = [jax.random.randint(jax.random.fold_in(own_key, axis), (), 0, length) for axis, length in enumerate(values.shape)]
    longest = values.shape.index(max(values.shape))
    beside = index_at[:longest] + [(index_at[longest] + 1) % values.shape[longest]] + index_at[longest + 1:]
    return values.at[tuple(index_at)].set(least).at[tuple(beside)].set(top_value)


def block_levels(own_key, dims, cuts, least, largest):
    gain, own = 1.0, jax.random.fold_in(own_key, 6)
    for axis_at, blocks in cuts:
        draws = jnp.exp(jax.random.uniform(jax.random.fold_in(own, axis_at), (blocks,), jnp.float32, least / len(cuts), largest / len(cuts)))
        gain = gain * jnp.repeat(draws, dims[axis_at] // blocks).reshape([-1 if axis == axis_at else 1 for axis in range(len(dims))])
    return gain


def normal_values(stream_key, extent, scale, limit, pieces=(), kind=jnp.bfloat16):
    factor_of = block_levels(stream_key, extent, pieces, -0.22, 0.18) if pieces else 1.0
    values = jax.random.normal(stream_key, extent, jnp.float32) * scale * factor_of
    return jnp.minimum(jnp.maximum(values, -limit), limit).astype(kind)


def setup_inputs(seed: int = 0) -> dict:
    streams_of = jax.random.split(jax.random.key(seed), 7)
    spectrum = normal_values(streams_of[0], (2, SCEN, SECTORS, GRID), 1.0, 6.0, ((2, 4), (3, 8)), jnp.float32)
    quantile_index = with_ends(jax.random.randint(streams_of[1], (SCEN,), GRID // 2, GRID - BANDS + 1), jax.random.fold_in(streams_of[1], 1), GRID // 2, GRID - BANDS).astype(jnp.int32)
    bands = with_ends(jax.random.randint(streams_of[2], (SLOTS,), 1, BANDS + 1), jax.random.fold_in(streams_of[2], 1), 1, BANDS).astype(jnp.int32)
    default_prob = jnp.clip(jnp.exp(math.log(0.1) - 3.912023 * jax.random.uniform(streams_of[3], (SLOTS,), jnp.float32) ** block_levels(streams_of[3], (SLOTS,), ((0, 32),), -0.2, 0.2)), 0.002, 0.1)
    weights = with_ends(jax.random.randint(streams_of[4], (SECTORS, SLOTS), 0, 9), jax.random.fold_in(streams_of[4], 1), 0, 8).astype(jnp.int32)
    live_rows = draw_live_rows(jax.random.fold_in(streams_of[6], 71), 0)
    return dict(spectrum=spectrum, quantile_index=quantile_index, bands=bands, default_prob=default_prob, weights=weights, live_rows=live_rows)


def reference(spectrum, quantile_index, bands, default_prob, weights, live_rows):
    loss_field = jnp.fft.ifft(spectrum[0] + 1j * spectrum[1], axis=2).real.astype(jnp.float32)
    suffix = jnp.cumsum(loss_field[:, :, ::-1], axis=2)[:, :, ::-1]
    targets = (quantile_index[:, None] - jnp.arange(1, BANDS + 1, dtype=jnp.int32)[None, :]).astype(jnp.int32)
    tables = jnp.take_along_axis(suffix, jnp.broadcast_to(targets[:, None, :], (SCEN, SECTORS, BANDS)), axis=2)
    slot_index = jnp.arange(SLOTS, dtype=jnp.int32)
    device_index = (slot_index // CAP).astype(jnp.int32)
    live_count = jnp.take(live_rows.reshape(-1), device_index)
    live_mask = (slot_index % CAP) < live_count
    exposure = bands.astype(jnp.float32)
    scaled = jnp.where(live_mask[None, :], weights.astype(jnp.float32) * (default_prob * exposure / 256.0)[None, :], jnp.float32(0.0))
    band_rows = (bands - 1).astype(jnp.int32)

    def one_scenario(table):
        product = scaled * jnp.take(table, band_rows, axis=1)
        return jnp.sum(product, axis=0), jnp.sum(product, axis=1)

    obligor_contrib, sector_sum = lax.map(one_scenario, tables)
    sector_share = sector_sum * (SECTORS / OBLIGORS)
    return (obligor_contrib, sector_share)
```

```python
import functools
import math

import jax
import jax.numpy as jnp
import numpy as np
from jax import lax
from jax.experimental import pallas as pl
from jax.experimental.pallas import tpu as pltpu
from jax.sharding import PartitionSpec as P

BANDS = 1024
OBL_DEV = 1024
LANES = 128
SUBS = 8
MESH = pl.DeviceIdType.MESH


def cos_sin(phase, grid_size):
    quarter = grid_size // 4
    shift = quarter.bit_length() - 1
    quad = (phase + quarter // 2) >> shift
    r = (phase - (quad << shift)).astype(jnp.float32) * (2.0 * math.pi / grid_size)
    r2 = r * r
    s = r * (1.0 + r2 * (-1 / 6 + r2 * (1 / 120 + r2 * (-1 / 5040 + r2 * (1 / 362880)))))
    c = 1.0 + r2 * (-0.5 + r2 * (1 / 24 + r2 * (-1 / 720 + r2 * (1 / 40320))))
    swap = (quad & 1) == 1
    sine = jnp.where(swap, c, s)
    cosine = jnp.where(swap, s, c)
    sine = jnp.where((quad & 2) == 2, -sine, sine)
    cosine = jnp.where(((quad + 1) & 2) == 2, -cosine, cosine)
    return cosine, sine


def kernel(
    dims,
    x_ref, q_ref, live_ref, bands_ref, prob_ref, w_ref,
    wh_hbm, wl_hbm, tw_hbm, cot_hbm,
    contrib_ref, share_ref,
    wh, wl, tw, cot, lhs_h, lhs_l, part, rs_buf, tabs, share_buf, share_send,
    const_sem, send_sem, rs_sem, ag_sem, sh_send_sem, sh_sem,
):
    grid_size, n_sector, n_obl, scen, sec_local = dims
    n_dev = n_sector * n_obl
    me_s = lax.axis_index("sector")
    me_o = lax.axis_index("obl")
    me = me_s * n_obl + me_o
    rows = x_ref.shape[2]
    a_count = rows // sec_local
    groups = rows // SUBS
    v_groups = BANDS // LANES
    row_groups = scen * sec_local // SUBS
    tiles = v_groups * row_groups
    own = tiles // n_obl
    c_per = SUBS // sec_local

    const_copies = [
        pltpu.make_async_copy(cot_hbm.at[me_o], cot, const_sem.at[0]),
        pltpu.make_async_copy(wh_hbm, wh, const_sem.at[1]),
        pltpu.make_async_copy(wl_hbm, wl, const_sem.at[2]),
        pltpu.make_async_copy(tw_hbm.at[me_o], tw, const_sem.at[3]),
    ]
    for copy in const_copies:
        copy.start()

    barrier = pltpu.get_barrier_semaphore()

    def greet(d, carry):
        peer = lax.rem(me + d, n_dev)
        pl.semaphore_signal(
            barrier, inc=1, device_id=(peer // n_obl, lax.rem(peer, n_obl)), device_id_type=MESH
        )
        return carry

    lax.fori_loop(1, n_dev, greet, 0)

    sub = lax.broadcasted_iota(jnp.int32, (SUBS, LANES), 0)
    lane = lax.broadcasted_iota(jnp.int32, (SUBS, LANES), 1)

    const_copies[0].wait()
    sub_a = lax.broadcasted_iota(jnp.int32, (rows, LANES), 0) // sec_local
    freq = me_o * (a_count * LANES) + sub_a * LANES + lax.broadcasted_iota(
        jnp.int32, (rows, LANES), 1
    )
    first = (freq == 0).astype(jnp.float32)
    half = (1.0 - first) * (0.5 / grid_size)

    def prepare(c, carry):
        p = q_ref[c] - BANDS
        cosine, sine = cos_sin((freq * p) & (grid_size - 1), grid_size)
        gc = cot[...]
        xr = x_ref[0, c]
        xi = x_ref[1, c]
        sr = xr * half - xi * gc
        si = xr * gc + xi * half
        yr = sr * cosine - si * sine
        yi = sr * sine + si * cosine
        rh = yr.astype(jnp.bfloat16)
        ih = yi.astype(jnp.bfloat16)
        rl = (yr - rh.astype(jnp.float32)).astype(jnp.bfloat16)
        il = (yi - ih.astype(jnp.float32)).astype(jnp.bfloat16)
        lhs_h[c, 0:rows, 0:LANES] = rh
        lhs_h[c, 0:rows, LANES:] = ih
        lhs_h[c, rows:, 0:LANES] = ih
        lhs_h[c, rows:, LANES:] = -rh
        lhs_l[c, 0:rows, 0:LANES] = rl
        lhs_l[c, 0:rows, LANES:] = il
        lhs_l[c, rows:, 0:LANES] = il
        lhs_l[c, rows:, LANES:] = -rl
        return carry

    lax.fori_loop(0, scen, prepare, 0)
    for copy in const_copies[1:]:
        copy.wait()

    v_step = 256
    tw_period = tw.shape[2]
    odd = (sub & (sec_local - 1)) == (sub // c_per)

    def transform(c, carry):
        p = q_ref[c] - BANDS
        xr = x_ref[0, c]
        xi = x_ref[1, c]
        sr = xr * half - xi * cot[...]
        offset = -sr.reshape(groups, SUBS, LANES).sum(axis=0)
        offset = jnp.sum(offset, axis=1, keepdims=True)
        zero = jnp.sum((xr * first)[0:SUBS], axis=1, keepdims=True) * (1.0 / grid_size)
        for v0 in range(0, BANDS, v_step):
            def dot(left, right):
                return jnp.dot(
                    left[c], right[:, v0:v0 + v_step], preferred_element_type=jnp.float32
                )
            field = dot(lhs_h, wh) + dot(lhs_h, wl) + dot(lhs_l, wh)
            t0 = v0 % tw_period
            turned = (
                field[0:rows] * tw[0, :, t0:t0 + v_step] - field[rows:] * tw[1, :, t0:t0 + v_step]
            )
            total = turned.reshape(groups, SUBS, v_step).sum(axis=0)
            for v in range(v_step // LANES):
                vg = v0 // LANES + v
                piece = total[:, v * LANES:(v + 1) * LANES]
                left_over = (grid_size - p - vg * LANES - lane).astype(jnp.float32)
                piece = piece + offset + zero * left_over
                shift = sec_local
                while shift < SUBS:
                    piece = piece + pltpu.roll(piece, shift, 0)
                    shift *= 2
                piece = jnp.where(odd, piece, pltpu.roll(piece, 1, 0))
                tile = vg * row_groups + c // c_per
                mask = (sub & (c_per - 1)) == lax.rem(c, c_per)
                part[tile] = jnp.where(mask, piece, part[tile])
        return carry

    part[...] = jnp.zeros_like(part)
    lax.fori_loop(0, scen, transform, 0)

    pl.semaphore_wait(barrier, n_dev - 1)

    def rs_copy(d):
        peer = lax.rem(me_o + d, n_obl)
        return pltpu.make_async_remote_copy(
            src_ref=part.at[pl.ds(peer * own, own)],
            dst_ref=rs_buf.at[me_o],
            send_sem=send_sem.at[0],
            recv_sem=rs_sem.at[d],
            device_id=(me_s, peer),
            device_id_type=MESH,
        )

    for d in range(1, n_obl):
        rs_copy(d).start()
    rs_buf[me_o] = part[pl.ds(me_o * own, own)]
    for d in range(1, n_obl):
        rs_copy(d).wait_recv()
    total = rs_buf[0]
    for i in range(1, n_obl):
        total = total + rs_buf[i]
    tabs[me_s, pl.ds(me_o * own, own)] = total

    def ag_copy(d):
        peer = lax.rem(me + d, n_dev)
        mine = tabs.at[me_s, pl.ds(me_o * own, own)]
        return pltpu.make_async_remote_copy(
            src_ref=mine,
            dst_ref=mine,
            send_sem=send_sem.at[1],
            recv_sem=ag_sem.at[d],
            device_id=(peer // n_obl, lax.rem(peer, n_obl)),
            device_id_type=MESH,
        )

    def each(copy_of, method, count):
        def step(d, carry):
            getattr(copy_of(d), method)()
            return carry
        lax.fori_loop(1, count, step, 0)

    each(ag_copy, "start", n_dev)
    each(ag_copy, "wait_recv", n_dev)

    live = live_ref[0, 0]
    cap_groups = bands_ref.shape[0]
    share_send[...] = jnp.zeros_like(share_send)
    high = sub >= c_per

    def look(g, carry):
        start = pl.multiple_of(g * LANES, LANES)
        band = jnp.broadcast_to(bands_ref[pl.ds(g, 1), :], (SUBS, LANES))
        prob = jnp.broadcast_to(prob_ref[pl.ds(g, 1), :], (SUBS, LANES))
        ok = (start + lane) < live
        band = jnp.where(ok, band, 1)
        amount = jnp.where(ok, prob * band.astype(jnp.float32) * (1.0 / 256.0), 0.0)
        at = BANDS - band
        low = at & (LANES - 1)
        top = at // LANES
        masks = [top == i for i in range(1, v_groups)]
        sums = [jnp.zeros((SUBS, LANES), jnp.float32) for _ in range(row_groups)]
        for s in range(n_sector):
            w0 = jnp.broadcast_to(w_ref[pl.ds(s * sec_local, 1), pl.ds(start, LANES)], (SUBS, LANES))
            w1 = jnp.broadcast_to(
                w_ref[pl.ds(s * sec_local + 1, 1), pl.ds(start, LANES)], (SUBS, LANES)
            )
            scaled = jnp.where(high, w1, w0).astype(jnp.float32) * amount
            for r in range(row_groups):
                found = jnp.take_along_axis(tabs[s, r], low, axis=1)
                for i in range(1, v_groups):
                    found = jnp.where(
                        masks[i - 1],
                        jnp.take_along_axis(tabs[s, i * row_groups + r], low, axis=1),
                        found,
                    )
                product = scaled * found
                share_send[s, r] += product
                sums[r] = sums[r] + product
        sums = [x + pltpu.roll(x, c_per, 0) for x in sums]
        contrib_ref[:, pl.ds(start, LANES)] = jnp.where(high, sums[1], sums[0])
        return carry

    lax.fori_loop(0, cap_groups, look, 0)

    for s in range(n_sector):
        packed = jnp.zeros((SUBS, LANES), jnp.float32)
        for r in range(row_groups):
            packed = jnp.where(lane == r, jnp.sum(share_send[s, r], axis=1, keepdims=True), packed)
        share_send[s, 0] = packed

    def sh_copy(d):
        peer = lax.rem(me + d, n_dev)
        peer_s = peer // n_obl
        return pltpu.make_async_remote_copy(
            src_ref=share_send.at[peer_s, 0],
            dst_ref=share_buf.at[me],
            send_sem=sh_send_sem,
            recv_sem=sh_sem.at[d],
            device_id=(peer_s, lax.rem(peer, n_obl)),
            device_id_type=MESH,
        )

    each(sh_copy, "start", n_dev)
    share_buf[me] = share_send[me_s, 0]
    each(sh_copy, "wait_recv", n_dev)
    share_ref[...] = jnp.sum(share_buf[...], axis=0)

    for d in range(1, n_obl):
        rs_copy(d).wait_send()
    each(ag_copy, "wait_send", n_dev)
    each(sh_copy, "wait_send", n_dev)


@functools.lru_cache(None)
def constants(grid_size, n_obl, sec_local):
    per_dev = grid_size // n_obl
    n_a = grid_size // LANES
    b = np.arange(LANES)
    v = np.arange(BANDS)
    angle = 2.0 * np.pi * (b[:, None] * v[None, :] % grid_size) / grid_size
    w = np.concatenate([np.cos(angle), -np.sin(angle)], axis=0).astype(np.float32)
    wh = w.astype(jnp.bfloat16)
    wl = (w - wh.astype(np.float32)).astype(jnp.bfloat16)
    period = min(n_a, BANDS)
    a = np.arange(n_a)
    turn = 2.0 * np.pi * (a[:, None] * np.arange(period)[None, :] % n_a) / n_a
    tw = np.stack([np.cos(turn), np.sin(turn)]).astype(np.float32)
    j = np.arange(grid_size, dtype=np.float64)
    cot = np.zeros(grid_size)
    cot[1:] = 0.5 / np.tan(np.pi * j[1:] / grid_size) / grid_size
    cot = cot.reshape(n_obl, per_dev // LANES, LANES).astype(np.float32)
    return wh, wl, tw, cot


def on_device(spectrum, quantile_index, bands, default_prob, weights, live_rows):
    _, scen, sec_local, per_dev = spectrum.shape
    n_obl = lax.axis_size("obl")
    n_sector = lax.axis_size("sector")
    n_dev = n_obl * n_sector
    grid_size = per_dev * n_obl
    a_count = per_dev // LANES
    rows = a_count * sec_local
    row_groups = scen * sec_local // SUBS
    tiles = BANDS // LANES * row_groups
    cap = bands.shape[0]
    wh, wl, tw, cot = constants(grid_size, n_obl, sec_local)
    period = tw.shape[2]
    tw = np.repeat(tw.reshape(2, n_obl, a_count, period).transpose(1, 0, 2, 3), sec_local, axis=2)
    cot = np.repeat(cot, sec_local, axis=1)
    x = spectrum.reshape(2, scen, sec_local, a_count, LANES)
    x = x.transpose(0, 1, 3, 2, 4).reshape(2, scen, rows, LANES)
    vmem = pl.BlockSpec(memory_space=pltpu.VMEM)
    smem = pl.BlockSpec(memory_space=pltpu.SMEM)
    hbm = pl.BlockSpec(memory_space=pl.ANY)
    f32, bf16 = jnp.float32, jnp.bfloat16
    contrib, share = pl.pallas_call(
        functools.partial(kernel, (grid_size, n_sector, n_obl, scen, sec_local)),
        out_shape=(
            jax.ShapeDtypeStruct((scen, cap), f32),
            jax.ShapeDtypeStruct((SUBS, LANES), f32),
        ),
        in_specs=[vmem, smem, smem, vmem, vmem, vmem, hbm, hbm, hbm, hbm],
        out_specs=(vmem, vmem),
        scratch_shapes=[
            pltpu.VMEM((2 * LANES, BANDS), bf16),
            pltpu.VMEM((2 * LANES, BANDS), bf16),
            pltpu.VMEM((2, rows, period), f32),
            pltpu.VMEM((rows, LANES), f32),
            pltpu.VMEM((scen, 2 * rows, 2 * LANES), bf16),
            pltpu.VMEM((scen, 2 * rows, 2 * LANES), bf16),
            pltpu.VMEM((tiles, SUBS, LANES), f32),
            pltpu.VMEM((n_obl, tiles // n_obl, SUBS, LANES), f32),
            pltpu.VMEM((n_sector, tiles, SUBS, LANES), f32),
            pltpu.VMEM((n_dev, SUBS, LANES), f32),
            pltpu.VMEM((n_sector, row_groups, SUBS, LANES), f32),
            pltpu.SemaphoreType.DMA((4,)),
            pltpu.SemaphoreType.DMA((2,)),
            pltpu.SemaphoreType.DMA((n_obl,)),
            pltpu.SemaphoreType.DMA((n_dev,)),
            pltpu.SemaphoreType.DMA,
            pltpu.SemaphoreType.DMA((n_dev,)),
        ],
        compiler_params=pltpu.CompilerParams(collective_id=0, has_side_effects=True),
    )(
        x, quantile_index, live_rows,
        bands.reshape(cap // LANES, LANES), default_prob.reshape(cap // LANES, LANES), weights,
        wh, wl, tw, cot,
    )
    obligors = OBL_DEV * n_sector * n_obl
    sectors = weights.shape[0]
    share = share[:, :row_groups].reshape(sec_local, SUBS // sec_local, row_groups)
    share = share.transpose(2, 1, 0).reshape(scen, sec_local)
    return contrib, share * (sectors / obligors)


def solution(mesh):
    in_specs = (
        P(None, None, "sector", "obl"),
        P(),
        P(("sector", "obl")),
        P(("sector", "obl")),
        P(None, ("sector", "obl")),
        P("sector", "obl"),
    )
    out_specs = (P(None, ("sector", "obl")), P(None, "sector"))
    return jax.shard_map(
        on_device, mesh=mesh, in_specs=in_specs, out_specs=out_specs, check_vma=False
    )
```

```python
import functools
import math

import jax
import jax.numpy as jnp
import numpy as np
from jax import lax
from jax.experimental import pallas as pl
from jax.experimental.pallas import tpu as pltpu
from jax.sharding import PartitionSpec as P

BANDS = 1024
OBL_DEV = 1024
LANES = 128
SUBS = 8
MESH = pl.DeviceIdType.MESH


def cos_sin(phase, grid_size):
    quarter = grid_size // 4
    shift = quarter.bit_length() - 1
    quad = (phase + quarter // 2) >> shift
    r = (phase - (quad << shift)).astype(jnp.float32) * (2.0 * math.pi / grid_size)
    r2 = r * r
    s = r * (1.0 + r2 * (-1 / 6 + r2 * (1 / 120 + r2 * (-1 / 5040 + r2 * (1 / 362880)))))
    c = 1.0 + r2 * (-0.5 + r2 * (1 / 24 + r2 * (-1 / 720 + r2 * (1 / 40320))))
    swap = (quad & 1) == 1
    sine = jnp.where(swap, c, s)
    cosine = jnp.where(swap, s, c)
    sine = jnp.where((quad & 2) == 2, -sine, sine)
    cosine = jnp.where(((quad + 1) & 2) == 2, -cosine, cosine)
    return cosine, sine


def kernel(
    dims,
    x_hbm, q_ref, live_ref, bands_hbm, prob_hbm, w_hbm, wh_hbm, wl_hbm, cot_hbm,
    contrib_ref, share_ref,
    x_ref, bands_ref, prob_ref, w_ref, rhs, tw, cot, lhs, part, rs_buf, tabs, hist_send, hist_buf,
    in_sem, x_sem, send_sem, rs_sem, ag_sem, sh_sem,
):
    grid_size, n_sector, n_obl, scen, sec_local = dims
    n_dev = n_sector * n_obl
    me_s = lax.axis_index("sector")
    me_o = lax.axis_index("obl")
    me = me_s * n_obl + me_o
    rows = x_ref.shape[2]
    a_count = rows // sec_local
    groups = rows // SUBS
    v_groups = BANDS // LANES
    row_groups = scen * sec_local // SUBS
    tiles = v_groups * row_groups
    own = tiles // n_obl
    c_per = SUBS // sec_local
    depth = 2 * LANES

    cot_copy = pltpu.make_async_copy(cot_hbm.at[me_o], cot, in_sem.at[0])
    x_copies = [
        pltpu.make_async_copy(x_hbm.at[:, pl.ds(h * (scen // 2), scen // 2)],
                              x_ref.at[:, pl.ds(h * (scen // 2), scen // 2)], x_sem.at[h])
        for h in range(2)
    ]
    rhs_copies = [
        pltpu.make_async_copy(wh_hbm, rhs.at[pl.ds(0, depth)], in_sem.at[1]),
        pltpu.make_async_copy(wl_hbm, rhs.at[pl.ds(depth, depth)], in_sem.at[2]),
    ]
    slot_copies = [
        pltpu.make_async_copy(bands_hbm, bands_ref, in_sem.at[3]),
        pltpu.make_async_copy(prob_hbm, prob_ref, in_sem.at[4]),
        pltpu.make_async_copy(w_hbm, w_ref, in_sem.at[5]),
    ]
    for copy in [cot_copy, *x_copies, *rhs_copies, *slot_copies]:
        copy.start()

    steps = [(ds, do) for ds in range(n_sector) for do in range(n_obl) if ds or do]
    steps.sort(key=lambda t: -(min(t[1], n_obl - t[1]) + min(t[0], n_sector - t[0])))

    def each(act, unrolled=n_dev <= 64):
        if unrolled:
            for ds, do in steps:
                act(ds, do)
        else:
            def step(d, carry):
                act(d // n_obl, lax.rem(d, n_obl))
                return carry
            lax.fori_loop(1, n_dev, step, 0)

    def peer_of(ds, do):
        return lax.rem(me_s + ds, n_sector), lax.rem(me_o + do, n_obl)

    barrier = pltpu.get_barrier_semaphore()
    each(lambda ds, do: pl.semaphore_signal(
        barrier, inc=1, device_id=peer_of(ds, do), device_id_type=MESH))

    sub = lax.broadcasted_iota(jnp.int32, (SUBS, LANES), 0)
    lane = lax.broadcasted_iota(jnp.int32, (SUBS, LANES), 1)

    tw_period = tw.shape[2]
    row_a = lax.broadcasted_iota(jnp.int32, (rows, LANES), 0) // sec_local + me_o * a_count
    row_lane = lax.broadcasted_iota(jnp.int32, (rows, LANES), 1)
    for v in range(tw_period // LANES):
        cosine, sine = cos_sin(
            (row_a * (row_lane + v * LANES)) & (tw_period - 1), tw_period
        )
        tw[0, :, v * LANES:(v + 1) * LANES] = cosine
        tw[1, :, v * LANES:(v + 1) * LANES] = sine

    freq = row_a * LANES + row_lane
    first = (freq == 0).astype(jnp.float32)
    half = (1.0 - first) * (0.5 / grid_size)

    def prepare(c, carry):
        p = q_ref[c] - BANDS
        cosine, sine = cos_sin((freq * p) & (grid_size - 1), grid_size)
        gc = cot[...]
        xr = x_ref[0, c]
        xi = x_ref[1, c]
        sr = xr * half - xi * gc
        si = xr * gc + xi * half
        yr = sr * cosine - si * sine
        yi = sr * sine + si * cosine
        rh = yr.astype(jnp.bfloat16)
        ih = yi.astype(jnp.bfloat16)
        rl = (yr - rh.astype(jnp.float32)).astype(jnp.bfloat16)
        il = (yi - ih.astype(jnp.float32)).astype(jnp.bfloat16)
        for k, (re, im) in enumerate(((rh, ih), (rh, ih), (rl, il))):
            at = k * depth
            lhs[c, 0:rows, at:at + LANES] = re
            lhs[c, 0:rows, at + LANES:at + depth] = im
            lhs[c, rows:, at:at + LANES] = im
            lhs[c, rows:, at + LANES:at + depth] = -re
        return carry

    cot_copy.wait()
    for h in range(2):
        x_copies[h].wait()
        lax.fori_loop(h * (scen // 2), (h + 1) * (scen // 2), prepare, 0)
    for copy in rhs_copies:
        copy.wait()
    rhs[2 * depth:, :] = rhs[0:depth, :]

    v_step = 256
    odd = (sub & (sec_local - 1)) == (sub // c_per)

    def transform(rg, carry):
        ends = []
        for i in range(c_per):
            c = rg * c_per + i
            xr = x_ref[0, c]
            sr = xr * half - x_ref[1, c] * cot[...]
            offset = -sr.reshape(groups, SUBS, LANES).sum(axis=0)
            offset = jnp.sum(offset, axis=1, keepdims=True)
            zero = jnp.sum((xr * first)[0:SUBS], axis=1, keepdims=True) * (1.0 / grid_size)
            ends.append((offset, zero, q_ref[c] - BANDS))
        left = lhs[pl.ds(rg * c_per, c_per)].reshape(c_per * 2 * rows, 3 * depth)
        for v0 in range(0, BANDS, v_step):
            field = jnp.dot(left, rhs[:, v0:v0 + v_step], preferred_element_type=jnp.float32)
            t0 = v0 % tw_period
            tile_of = [jnp.zeros((SUBS, LANES), jnp.float32)] * (v_step // LANES)
            for i in range(c_per):
                offset, zero, p = ends[i]
                at = i * 2 * rows
                turned = (
                    field[at:at + rows] * tw[0, :, t0:t0 + v_step]
                    - field[at + rows:at + 2 * rows] * tw[1, :, t0:t0 + v_step]
                )
                total = turned.reshape(groups, SUBS, v_step).sum(axis=0)
                for v in range(v_step // LANES):
                    piece = total[:, v * LANES:(v + 1) * LANES]
                    left_over = (grid_size - p - v0 - v * LANES - lane).astype(jnp.float32)
                    piece = piece + offset + zero * left_over
                    shift = sec_local
                    while shift < SUBS:
                        piece = piece + pltpu.roll(piece, shift, 0)
                        shift *= 2
                    piece = jnp.where(odd, piece, pltpu.roll(piece, 1, 0))
                    tile_of[v] = jnp.where((sub & (c_per - 1)) == i, piece, tile_of[v])
            for v in range(v_step // LANES):
                part[(v0 // LANES + v) * row_groups + rg] = tile_of[v]
        return carry

    lax.fori_loop(0, row_groups, transform, 0)

    pl.semaphore_wait(barrier, n_dev - 1)

    def rs_copy(d):
        peer = lax.rem(me_o + d, n_obl)
        return pltpu.make_async_remote_copy(
            src_ref=part.at[pl.ds(peer * own, own)],
            dst_ref=rs_buf.at[me_o],
            send_sem=send_sem.at[0],
            recv_sem=rs_sem.at[d],
            device_id=(me_s, peer),
            device_id_type=MESH,
        )

    for d in sorted(range(1, n_obl), key=lambda d: -min(d, n_obl - d)):
        rs_copy(d).start()
    rs_buf[me_o] = part[pl.ds(me_o * own, own)]
    for d in range(1, n_obl):
        rs_copy(d).wait_recv()
    total = rs_buf[0]
    for i in range(1, n_obl):
        total = total + rs_buf[i]
    tabs[me_s, pl.ds(me_o * own, own)] = total

    def ag_copy(ds, do):
        mine = tabs.at[me_s, pl.ds(me_o * own, own)]
        return pltpu.make_async_remote_copy(
            src_ref=mine,
            dst_ref=mine,
            send_sem=send_sem.at[1],
            recv_sem=ag_sem.at[ds * n_obl + do],
            device_id=peer_of(ds, do),
            device_id_type=MESH,
        )

    each(lambda ds, do: ag_copy(ds, do).start())

    for copy in slot_copies:
        copy.wait()
    live = live_ref[0, 0]
    cap_groups = bands_ref.shape[0]

    def slots(g, size):
        band = bands_ref[pl.ds(g, 1), :]
        prob = prob_ref[pl.ds(g, 1), :]
        ok = (g * LANES + lax.broadcasted_iota(jnp.int32, (1, LANES), 1)) < live
        band = jnp.where(ok, band, 1)
        amount = jnp.where(ok, prob * band.astype(jnp.float32) * (1.0 / 256.0), 0.0)
        return jnp.broadcast_to(BANDS - band, (size, LANES)), amount

    def count(g, sums):
        ats, lefts = [], []
        for i in range(2):
            at, amount = slots(2 * g + i, BANDS)
            start = pl.multiple_of((2 * g + i) * LANES, LANES)
            scaled = w_ref[:, pl.ds(start, LANES)].astype(jnp.float32) * amount
            split = []
            for _ in range(3):
                piece = scaled.astype(jnp.bfloat16).astype(jnp.float32)
                split.append(piece)
                scaled = scaled - piece
            lefts.append(jnp.concatenate(split, axis=0))
            ats.append(at)
        at = jnp.concatenate(ats, axis=1)
        left = jnp.concatenate(lefts, axis=1).astype(jnp.bfloat16)
        spot = lax.broadcasted_iota(jnp.int32, (BANDS, 2 * LANES), 0)
        hot = jnp.where(at == spot, 1.0, 0.0).astype(jnp.bfloat16)
        return sums + lax.dot_general(
            left, hot, (((1,), (1,)), ((), ())), preferred_element_type=jnp.float32
        )

    sectors = w_ref.shape[0]
    sums = jnp.zeros((3 * sectors, BANDS), jnp.float32)
    sums = lax.fori_loop(0, cap_groups // 2, count, sums)
    hist = sums[0:sectors] + sums[sectors:2 * sectors] + sums[2 * sectors:]
    for s in range(n_sector):
        hist_send[s] = hist[s * sec_local:(s + 1) * sec_local]

    def sh_copy(ds, do):
        peer = peer_of(ds, do)
        return pltpu.make_async_remote_copy(
            src_ref=hist_send.at[peer[0]],
            dst_ref=hist_buf.at[me],
            send_sem=send_sem.at[2],
            recv_sem=sh_sem.at[ds * n_obl + do],
            device_id=peer,
            device_id_type=MESH,
        )

    each(lambda ds, do: sh_copy(ds, do).start())
    hist_buf[me] = hist_send[me_s]
    each(lambda ds, do: ag_copy(ds, do).wait_recv())

    high = sub >= c_per

    def look(g, carry):
        start = pl.multiple_of(g * LANES, LANES)
        at, amount = slots(g, SUBS)
        amount = jnp.broadcast_to(amount, (SUBS, LANES))
        low = at & (LANES - 1)
        top = at // LANES
        masks = [top == i for i in range(1, v_groups)]
        sums = [jnp.zeros((SUBS, LANES), jnp.float32) for _ in range(row_groups)]
        for s in range(n_sector):
            w0, w1 = (
                jnp.broadcast_to(
                    w_ref[pl.ds(s * sec_local + k, 1), pl.ds(start, LANES)], (SUBS, LANES)
                )
                for k in range(2)
            )
            scaled = jnp.where(high, w1, w0).astype(jnp.float32) * amount
            for r in range(row_groups):
                found = jnp.take_along_axis(tabs[s, r], low, axis=1)
                for i in range(1, v_groups):
                    found = jnp.where(
                        masks[i - 1],
                        jnp.take_along_axis(tabs[s, i * row_groups + r], low, axis=1),
                        found,
                    )
                sums[r] = sums[r] + scaled * found
        sums = [x + pltpu.roll(x, c_per, 0) for x in sums]
        contrib_ref[:, pl.ds(start, LANES)] = jnp.where(high, sums[1], sums[0])
        return carry

    lax.fori_loop(0, cap_groups, look, 0)

    each(lambda ds, do: sh_copy(ds, do).wait_recv())
    hist = jnp.sum(hist_buf[...], axis=0)
    spread = jnp.zeros((SUBS, LANES), jnp.float32)
    for r in range(row_groups):
        total = jnp.zeros((SUBS, LANES), jnp.float32)
        for v in range(v_groups):
            h0, h1 = (
                jnp.broadcast_to(hist[k:k + 1, v * LANES:(v + 1) * LANES], (SUBS, LANES))
                for k in range(2)
            )
            total = total + tabs[me_s, v * row_groups + r] * jnp.where(high, h1, h0)
        total = jnp.sum(total, axis=1, keepdims=True)
        spread = jnp.where(lane == r * c_per + (sub & (c_per - 1)), total, spread)
    spread = spread * (sectors / (OBL_DEV * n_dev))
    for k in range(sec_local):
        row = jnp.sum(jnp.where(sub // c_per == k, spread, 0.0), axis=0, keepdims=True)
        share_ref[k:k + 1, :] = row[:, 0:scen]

    for d in range(1, n_obl):
        rs_copy(d).wait_send()
    each(lambda ds, do: ag_copy(ds, do).wait_send())
    each(lambda ds, do: sh_copy(ds, do).wait_send())


@functools.lru_cache(None)
def constants(grid_size, n_obl, sec_local):
    per_dev = grid_size // n_obl
    b = np.arange(LANES)
    v = np.arange(BANDS)
    angle = 2.0 * np.pi * (b[:, None] * v[None, :] % grid_size) / grid_size
    w = np.concatenate([np.cos(angle), -np.sin(angle)], axis=0).astype(np.float32)
    wh = w.astype(jnp.bfloat16)
    wl = (w - wh.astype(np.float32)).astype(jnp.bfloat16)
    j = np.arange(grid_size, dtype=np.float64)
    cot = np.zeros(grid_size)
    cot[1:] = 0.5 / np.tan(np.pi * j[1:] / grid_size) / grid_size
    cot = cot.reshape(n_obl, per_dev // LANES, LANES).astype(np.float32)
    return wh, wl, cot


def on_device(spectrum, quantile_index, bands, default_prob, weights, live_rows):
    _, scen, sec_local, per_dev = spectrum.shape
    n_obl = lax.axis_size("obl")
    n_sector = lax.axis_size("sector")
    n_dev = n_obl * n_sector
    grid_size = per_dev * n_obl
    a_count = per_dev // LANES
    rows = a_count * sec_local
    row_groups = scen * sec_local // SUBS
    tiles = BANDS // LANES * row_groups
    cap = bands.shape[0]
    wh, wl, cot = constants(grid_size, n_obl, sec_local)
    period = grid_size // LANES
    cot = np.repeat(cot, sec_local, axis=1)
    x = spectrum.reshape(2, scen, sec_local, a_count, LANES)
    x = x.transpose(0, 1, 3, 2, 4).reshape(2, scen, rows, LANES)
    vmem = pl.BlockSpec(memory_space=pltpu.VMEM)
    smem = pl.BlockSpec(memory_space=pltpu.SMEM)
    hbm = pl.BlockSpec(memory_space=pl.ANY)
    f32, bf16 = jnp.float32, jnp.bfloat16
    contrib, share = pl.pallas_call(
        functools.partial(kernel, (grid_size, n_sector, n_obl, scen, sec_local)),
        out_shape=(
            jax.ShapeDtypeStruct((scen, cap), f32),
            jax.ShapeDtypeStruct((sec_local, scen), f32),
        ),
        in_specs=[hbm, smem, smem, hbm, hbm, hbm, hbm, hbm, hbm],
        out_specs=(vmem, vmem),
        scratch_shapes=[
            pltpu.VMEM(x.shape, f32),
            pltpu.VMEM((cap // LANES, LANES), jnp.int32),
            pltpu.VMEM((cap // LANES, LANES), f32),
            pltpu.VMEM(weights.shape, jnp.int32),
            pltpu.VMEM((6 * LANES, BANDS), bf16),
            pltpu.VMEM((2, rows, period), f32),
            pltpu.VMEM((rows, LANES), f32),
            pltpu.VMEM((scen, 2 * rows, 6 * LANES), bf16),
            pltpu.VMEM((tiles, SUBS, LANES), f32),
            pltpu.VMEM((n_obl, tiles // n_obl, SUBS, LANES), f32),
            pltpu.VMEM((n_sector, tiles, SUBS, LANES), f32),
            pltpu.VMEM((n_sector, sec_local, BANDS), f32),
            pltpu.VMEM((n_dev, sec_local, BANDS), f32),
            pltpu.SemaphoreType.DMA((6,)),
            pltpu.SemaphoreType.DMA((2,)),
            pltpu.SemaphoreType.DMA((3,)),
            pltpu.SemaphoreType.DMA((n_obl,)),
            pltpu.SemaphoreType.DMA((n_dev,)),
            pltpu.SemaphoreType.DMA((n_dev,)),
        ],
        compiler_params=pltpu.CompilerParams(
            collective_id=0, has_side_effects=True, vmem_limit_bytes=40 * 1024 * 1024
        ),
    )(
        x, quantile_index, live_rows,
        bands.reshape(cap // LANES, LANES), default_prob.reshape(cap // LANES, LANES), weights,
        wh, wl, cot,
    )
    return contrib, share.T


def solution(mesh):
    in_specs = (
        P(None, None, "sector", "obl"),
        P(),
        P(("sector", "obl")),
        P(("sector", "obl")),
        P(None, ("sector", "obl")),
        P("sector", "obl"),
    )
    out_specs = (P(None, ("sector", "obl")), P(None, "sector"))
    return jax.shard_map(
        on_device, mesh=mesh, in_specs=in_specs, out_specs=out_specs, check_vma=False
    )
```

```python
import functools
import math

import jax
import jax.numpy as jnp
import numpy as np
from jax import lax
from jax.experimental import pallas as pl
from jax.experimental.pallas import tpu as pltpu
from jax.sharding import PartitionSpec as P

BANDS = 1024
OBL_DEV = 1024
LANES = 128
SUBS = 8
MESH = pl.DeviceIdType.MESH


def cos_sin(phase, grid_size):
    quarter = grid_size // 4
    shift = quarter.bit_length() - 1
    quad = (phase + quarter // 2) >> shift
    r = (phase - (quad << shift)).astype(jnp.float32) * (2.0 * math.pi / grid_size)
    r2 = r * r
    s = r * (1.0 + r2 * (-1 / 6 + r2 * (1 / 120 + r2 * (-1 / 5040 + r2 * (1 / 362880)))))
    c = 1.0 + r2 * (-0.5 + r2 * (1 / 24 + r2 * (-1 / 720 + r2 * (1 / 40320))))
    swap = (quad & 1) == 1
    sine = jnp.where(swap, c, s)
    cosine = jnp.where(swap, s, c)
    sine = jnp.where((quad & 2) == 2, -sine, sine)
    cosine = jnp.where(((quad + 1) & 2) == 2, -cosine, cosine)
    return cosine, sine


def kernel(
    dims,
    x_hbm, q_ref, live_ref, bands_hbm, prob_hbm, w_hbm, wh_hbm, wl_hbm, cot_hbm,
    contrib_ref, share_ref,
    x_ref, bands_ref, prob_ref, w_ref, rhs, tw, cot, lhs, part, rs_buf, tabs, hist_send, hist_buf,
    in_sem, x_sem, send_sem, rs_sem, ag_sem, sh_sem,
):
    grid_size, n_sector, n_obl, scen, sec_local = dims
    n_dev = n_sector * n_obl
    me_s = lax.axis_index("sector")
    me_o = lax.axis_index("obl")
    me = me_s * n_obl + me_o
    rows = x_ref.shape[2]
    a_count = rows // sec_local
    groups = rows // SUBS
    v_groups = BANDS // LANES
    row_groups = scen * sec_local // SUBS
    tiles = v_groups * row_groups
    own = tiles // n_obl
    c_per = SUBS // sec_local
    depth = 2 * LANES

    cot_copy = pltpu.make_async_copy(cot_hbm.at[me_o], cot, in_sem.at[0])
    x_copies = [
        pltpu.make_async_copy(x_hbm.at[:, pl.ds(h * (scen // 2), scen // 2)],
                              x_ref.at[:, pl.ds(h * (scen // 2), scen // 2)], x_sem.at[h])
        for h in range(2)
    ]
    rhs_copies = [
        pltpu.make_async_copy(wh_hbm, rhs.at[pl.ds(0, depth)], in_sem.at[1]),
        pltpu.make_async_copy(wl_hbm, rhs.at[pl.ds(depth, depth)], in_sem.at[2]),
    ]
    slot_copies = [
        pltpu.make_async_copy(bands_hbm, bands_ref, in_sem.at[3]),
        pltpu.make_async_copy(prob_hbm, prob_ref, in_sem.at[4]),
        pltpu.make_async_copy(w_hbm, w_ref, in_sem.at[5]),
    ]
    for copy in [cot_copy, *x_copies, *rhs_copies, *slot_copies]:
        copy.start()

    steps = [(ds, do) for ds in range(n_sector) for do in range(n_obl) if ds or do]
    steps.sort(key=lambda t: -(min(t[1], n_obl - t[1]) + min(t[0], n_sector - t[0])))

    def each(act, unrolled=n_dev <= 64):
        if unrolled:
            for ds, do in steps:
                act(ds, do)
        else:
            def step(d, carry):
                act(d // n_obl, lax.rem(d, n_obl))
                return carry
            lax.fori_loop(1, n_dev, step, 0)

    def peer_of(ds, do):
        return lax.rem(me_s + ds, n_sector), lax.rem(me_o + do, n_obl)

    barrier = pltpu.get_barrier_semaphore()
    each(lambda ds, do: pl.semaphore_signal(
        barrier, inc=1, device_id=peer_of(ds, do), device_id_type=MESH))

    sub = lax.broadcasted_iota(jnp.int32, (SUBS, LANES), 0)
    lane = lax.broadcasted_iota(jnp.int32, (SUBS, LANES), 1)

    tw_period = tw.shape[2]
    row_a = lax.broadcasted_iota(jnp.int32, (rows, LANES), 0) // sec_local + me_o * a_count
    row_lane = lax.broadcasted_iota(jnp.int32, (rows, LANES), 1)
    for v in range(tw_period // LANES):
        cosine, sine = cos_sin(
            (row_a * (row_lane + v * LANES)) & (tw_period - 1), tw_period
        )
        tw[0, :, v * LANES:(v + 1) * LANES] = cosine
        tw[1, :, v * LANES:(v + 1) * LANES] = sine

    freq = row_a * LANES + row_lane
    first = (freq == 0).astype(jnp.float32)
    half = (1.0 - first) * (0.5 / grid_size)

    def prepare(c, carry):
        p = q_ref[c] - BANDS
        cosine, sine = cos_sin((freq * p) & (grid_size - 1), grid_size)
        gc = cot[...]
        xr = x_ref[0, c]
        xi = x_ref[1, c]
        sr = xr * half - xi * gc
        si = xr * gc + xi * half
        yr = sr * cosine - si * sine
        yi = sr * sine + si * cosine
        rh = yr.astype(jnp.bfloat16)
        ih = yi.astype(jnp.bfloat16)
        rl = (yr - rh.astype(jnp.float32)).astype(jnp.bfloat16)
        il = (yi - ih.astype(jnp.float32)).astype(jnp.bfloat16)
        for k, (re, im) in enumerate(((rh, ih), (rh, ih), (rl, il))):
            at = k * depth
            lhs[c, 0:rows, at:at + LANES] = re
            lhs[c, 0:rows, at + LANES:at + depth] = im
            lhs[c, rows:, at:at + LANES] = im
            lhs[c, rows:, at + LANES:at + depth] = -re
        return carry

    cot_copy.wait()
    for h in range(2):
        x_copies[h].wait()
        lax.fori_loop(h * (scen // 2), (h + 1) * (scen // 2), prepare, 0)
    for copy in rhs_copies:
        copy.wait()
    rhs[2 * depth:, :] = rhs[0:depth, :]

    v_step = 256
    odd = (sub & (sec_local - 1)) == (sub // c_per)

    def transform(rg, carry):
        ends = []
        for i in range(c_per):
            c = rg * c_per + i
            xr = x_ref[0, c]
            sr = xr * half - x_ref[1, c] * cot[...]
            offset = -sr.reshape(groups, SUBS, LANES).sum(axis=0)
            offset = jnp.sum(offset, axis=1, keepdims=True)
            zero = jnp.sum((xr * first)[0:SUBS], axis=1, keepdims=True) * (1.0 / grid_size)
            ends.append((offset, zero, q_ref[c] - BANDS))
        left = lhs[pl.ds(rg * c_per, c_per)].reshape(c_per * 2 * rows, 3 * depth)
        for v0 in range(0, BANDS, v_step):
            field = jnp.dot(left, rhs[:, v0:v0 + v_step], preferred_element_type=jnp.float32)
            t0 = v0 % tw_period
            tile_of = [jnp.zeros((SUBS, LANES), jnp.float32)] * (v_step // LANES)
            for i in range(c_per):
                offset, zero, p = ends[i]
                at = i * 2 * rows
                turned = (
                    field[at:at + rows] * tw[0, :, t0:t0 + v_step]
                    - field[at + rows:at + 2 * rows] * tw[1, :, t0:t0 + v_step]
                )
                total = turned.reshape(groups, SUBS, v_step).sum(axis=0)
                for v in range(v_step // LANES):
                    piece = total[:, v * LANES:(v + 1) * LANES]
                    left_over = (grid_size - p - v0 - v * LANES - lane).astype(jnp.float32)
                    piece = piece + offset + zero * left_over
                    shift = sec_local
                    while shift < SUBS:
                        piece = piece + pltpu.roll(piece, shift, 0)
                        shift *= 2
                    piece = jnp.where(odd, piece, pltpu.roll(piece, 1, 0))
                    tile_of[v] = jnp.where((sub & (c_per - 1)) == i, piece, tile_of[v])
            for v in range(v_step // LANES):
                part[(v0 // LANES + v) * row_groups + rg] = tile_of[v]
        return carry

    lax.fori_loop(0, row_groups, transform, 0)

    pl.semaphore_wait(barrier, n_dev - 1)

    def rs_copy(d):
        peer = lax.rem(me_o + d, n_obl)
        return pltpu.make_async_remote_copy(
            src_ref=part.at[pl.ds(peer * own, own)],
            dst_ref=rs_buf.at[me_o],
            send_sem=send_sem.at[0],
            recv_sem=rs_sem.at[d],
            device_id=(me_s, peer),
            device_id_type=MESH,
        )

    for d in sorted(range(1, n_obl), key=lambda d: -min(d, n_obl - d)):
        rs_copy(d).start()
    rs_buf[me_o] = part[pl.ds(me_o * own, own)]
    for d in range(1, n_obl):
        rs_copy(d).wait_recv()
    total = rs_buf[0]
    for i in range(1, n_obl):
        total = total + rs_buf[i]
    tabs[me_s, pl.ds(me_o * own, own)] = total

    def ag_copy(ds, do):
        mine = tabs.at[me_s, pl.ds(me_o * own, own)]
        return pltpu.make_async_remote_copy(
            src_ref=mine,
            dst_ref=mine,
            send_sem=send_sem.at[1],
            recv_sem=ag_sem.at[ds * n_obl + do],
            device_id=peer_of(ds, do),
            device_id_type=MESH,
        )

    each(lambda ds, do: ag_copy(ds, do).start())

    for copy in slot_copies:
        copy.wait()
    live = live_ref[0]
    cap_groups = bands_ref.shape[0]

    def slots(g, size):
        band = bands_ref[pl.ds(g, 1), :]
        prob = prob_ref[pl.ds(g, 1), :]
        ok = (g * LANES + lax.broadcasted_iota(jnp.int32, (1, LANES), 1)) < live
        band = jnp.where(ok, band, 1)
        amount = jnp.where(ok, prob * band.astype(jnp.float32) * (1.0 / 256.0), 0.0)
        return jnp.broadcast_to(BANDS - band, (size, LANES)), amount

    def count(g, sums):
        ats, lefts = [], []
        for i in range(2):
            at, amount = slots(2 * g + i, BANDS)
            start = pl.multiple_of((2 * g + i) * LANES, LANES)
            scaled = w_ref[:, pl.ds(start, LANES)].astype(jnp.float32) * amount
            split = []
            for _ in range(3):
                piece = scaled.astype(jnp.bfloat16).astype(jnp.float32)
                split.append(piece)
                scaled = scaled - piece
            lefts.append(jnp.concatenate(split, axis=0))
            ats.append(at)
        at = jnp.concatenate(ats, axis=1)
        left = jnp.concatenate(lefts, axis=1).astype(jnp.bfloat16)
        spot = lax.broadcasted_iota(jnp.int32, (BANDS, 2 * LANES), 0)
        hot = jnp.where(at == spot, 1.0, 0.0).astype(jnp.bfloat16)
        return sums + lax.dot_general(
            left, hot, (((1,), (1,)), ((), ())), preferred_element_type=jnp.float32
        )

    sectors = w_ref.shape[0]
    sums = jnp.zeros((3 * sectors, BANDS), jnp.float32)
    sums = lax.fori_loop(0, cap_groups // 2, count, sums)
    hist = sums[0:sectors] + sums[sectors:2 * sectors] + sums[2 * sectors:]
    for s in range(n_sector):
        hist_send[s] = hist[s * sec_local:(s + 1) * sec_local]

    def sh_copy(ds, do):
        peer = peer_of(ds, do)
        return pltpu.make_async_remote_copy(
            src_ref=hist_send.at[peer[0]],
            dst_ref=hist_buf.at[me],
            send_sem=send_sem.at[2],
            recv_sem=sh_sem.at[ds * n_obl + do],
            device_id=peer,
            device_id_type=MESH,
        )

    each(lambda ds, do: sh_copy(ds, do).start())
    hist_buf[me] = hist_send[me_s]
    each(lambda ds, do: ag_copy(ds, do).wait_recv())

    high = sub >= c_per

    def look(g, carry):
        start = pl.multiple_of(g * LANES, LANES)
        at, amount = slots(g, SUBS)
        amount = jnp.broadcast_to(amount, (SUBS, LANES))
        low = at & (LANES - 1)
        top = at // LANES
        masks = [top == i for i in range(1, v_groups)]
        sums = [jnp.zeros((SUBS, LANES), jnp.float32) for _ in range(row_groups)]
        for s in range(n_sector):
            w0, w1 = (
                jnp.broadcast_to(
                    w_ref[pl.ds(s * sec_local + k, 1), pl.ds(start, LANES)], (SUBS, LANES)
                )
                for k in range(2)
            )
            scaled = jnp.where(high, w1, w0).astype(jnp.float32) * amount
            for r in range(row_groups):
                found = jnp.take_along_axis(tabs[s, r], low, axis=1)
                for i in range(1, v_groups):
                    found = jnp.where(
                        masks[i - 1],
                        jnp.take_along_axis(tabs[s, i * row_groups + r], low, axis=1),
                        found,
                    )
                sums[r] = sums[r] + scaled * found
        sums = [x + pltpu.roll(x, c_per, 0) for x in sums]
        contrib_ref[:, pl.ds(start, LANES)] = jnp.where(high, sums[1], sums[0])
        return carry

    lax.fori_loop(0, cap_groups, look, 0, unroll=2)

    each(lambda ds, do: sh_copy(ds, do).wait_recv())
    hist = jnp.sum(hist_buf[...], axis=0)
    spread = jnp.zeros((SUBS, LANES), jnp.float32)
    for r in range(row_groups):
        total = jnp.zeros((SUBS, LANES), jnp.float32)
        for v in range(v_groups):
            h0, h1 = (
                jnp.broadcast_to(hist[k:k + 1, v * LANES:(v + 1) * LANES], (SUBS, LANES))
                for k in range(2)
            )
            total = total + tabs[me_s, v * row_groups + r] * jnp.where(high, h1, h0)
        total = jnp.sum(total, axis=1, keepdims=True)
        spread = jnp.where(lane == r * c_per + (sub & (c_per - 1)), total, spread)
    spread = spread * (sectors / (OBL_DEV * n_dev))
    for k in range(sec_local):
        row = jnp.sum(jnp.where(sub // c_per == k, spread, 0.0), axis=0, keepdims=True)
        share_ref[k:k + 1, :] = row[:, 0:scen]

    for d in range(1, n_obl):
        rs_copy(d).wait_send()
    each(lambda ds, do: ag_copy(ds, do).wait_send())
    each(lambda ds, do: sh_copy(ds, do).wait_send())


@functools.lru_cache(None)
def constants(grid_size, n_obl, sec_local):
    per_dev = grid_size // n_obl
    b = np.arange(LANES)
    v = np.arange(BANDS)
    angle = 2.0 * np.pi * (b[:, None] * v[None, :] % grid_size) / grid_size
    w = np.concatenate([np.cos(angle), -np.sin(angle)], axis=0).astype(np.float32)
    wh = w.astype(jnp.bfloat16)
    wl = (w - wh.astype(np.float32)).astype(jnp.bfloat16)
    j = np.arange(grid_size, dtype=np.float64)
    cot = np.zeros(grid_size)
    cot[1:] = 0.5 / np.tan(np.pi * j[1:] / grid_size) / grid_size
    cot = cot.reshape(n_obl, per_dev // LANES, LANES).astype(np.float32)
    return wh, wl, cot


def on_device(spectrum, quantile_index, bands, default_prob, weights, live_rows):
    _, scen, sec_local, per_dev = spectrum.shape
    n_obl = lax.axis_size("obl")
    n_sector = lax.axis_size("sector")
    n_dev = n_obl * n_sector
    grid_size = per_dev * n_obl
    a_count = per_dev // LANES
    rows = a_count * sec_local
    row_groups = scen * sec_local // SUBS
    tiles = BANDS // LANES * row_groups
    cap = bands.shape[0]
    wh, wl, cot = constants(grid_size, n_obl, sec_local)
    period = grid_size // LANES
    cot = np.repeat(cot, sec_local, axis=1)
    x = spectrum.reshape(2, scen, sec_local, a_count, LANES)
    x = x.transpose(0, 1, 3, 2, 4).reshape(2, scen, rows, LANES)
    vmem = pl.BlockSpec(memory_space=pltpu.VMEM)
    smem = pl.BlockSpec(memory_space=pltpu.SMEM)
    hbm = pl.BlockSpec(memory_space=pl.ANY)
    f32, bf16 = jnp.float32, jnp.bfloat16
    contrib, share = pl.pallas_call(
        functools.partial(kernel, (grid_size, n_sector, n_obl, scen, sec_local)),
        out_shape=(
            jax.ShapeDtypeStruct((scen, cap), f32),
            jax.ShapeDtypeStruct((sec_local, scen), f32),
        ),
        in_specs=[hbm, smem, smem, hbm, hbm, hbm, hbm, hbm, hbm],
        out_specs=(vmem, vmem),
        scratch_shapes=[
            pltpu.VMEM(x.shape, f32),
            pltpu.VMEM((cap // LANES, LANES), jnp.int32),
            pltpu.VMEM((cap // LANES, LANES), f32),
            pltpu.VMEM(weights.shape, jnp.int32),
            pltpu.VMEM((6 * LANES, BANDS), bf16),
            pltpu.VMEM((2, rows, period), f32),
            pltpu.VMEM((rows, LANES), f32),
            pltpu.VMEM((scen, 2 * rows, 6 * LANES), bf16),
            pltpu.VMEM((tiles, SUBS, LANES), f32),
            pltpu.VMEM((n_obl, tiles // n_obl, SUBS, LANES), f32),
            pltpu.VMEM((n_sector, tiles, SUBS, LANES), f32),
            pltpu.VMEM((n_sector, sec_local, BANDS), f32),
            pltpu.VMEM((n_dev, sec_local, BANDS), f32),
            pltpu.SemaphoreType.DMA((6,)),
            pltpu.SemaphoreType.DMA((2,)),
            pltpu.SemaphoreType.DMA((3,)),
            pltpu.SemaphoreType.DMA((n_obl,)),
            pltpu.SemaphoreType.DMA((n_dev,)),
            pltpu.SemaphoreType.DMA((n_dev,)),
        ],
        compiler_params=pltpu.CompilerParams(
            collective_id=0, has_side_effects=True
        ),
    )(
        x, quantile_index, live_rows.reshape(1),
        bands.reshape(cap // LANES, LANES), default_prob.reshape(cap // LANES, LANES), weights,
        wh, wl, cot,
    )
    return contrib, share.T


def solution(mesh):
    in_specs = (
        P(None, None, "sector", "obl"),
        P(),
        P(("sector", "obl")),
        P(("sector", "obl")),
        P(None, ("sector", "obl")),
        P("sector", "obl"),
    )
    out_specs = (P(None, ("sector", "obl")), P(None, "sector"))
    return jax.shard_map(
        on_device, mesh=mesh, in_specs=in_specs, out_specs=out_specs, check_vma=False
    )
```
